32 devices in a mesh: dp: 16 (over z, y, x), head: 2 (over core).
Axes of the slice: x: 2, y: 2, z: 4, core: 2. Of those that a mesh axis runs over, the one named last changes fastest.
Arguments:
- hidden: bfloat16 [64, 512, 3584], P(('dp', 'head')), may hold values from -6 to 6
- head_proj: bfloat16 [4, 3584, 128], P('head'), may hold values from -0.09375 to 0.09375
- head_out: bfloat16 [4, 128], P('head'), may hold values from -0.8984375 to 0.8984375
- head_ratio: int32 [4], replicated, may hold values from 2 to 7
- group_of: int32 [64], replicated, may hold values from 0 to 3, as said below
- lengths: int32 [64], P(('dp', 'head')), may hold values from 1 to 512
- token_mask: int32 [64, 512], P(('dp', 'head')), may hold values 0 or 1
Outputs:
- advantages: float32 [64, 512], P(('dp', 'head'))
The draws below stay inside these ranges and needn't reach their ends.
Inputs may be any that keep to these rules, and one draw needn't show every extreme that they name: `group_of`: every one of the 4 groups holds exactly 16 rollouts.
All inputs are finite; a program needn't handle non-finite values. No bound on the sum of `token_mask` on one device may be relied on, other than what follows from the above.
Results may differ from the reference program's by a relative error of at most 0.0026.
Values may be sent and summed in bfloat16 or wider, within the bound.
No kernel may reach another device: no remote copies, remote signals or barrier semaphores. Data moves between devices by JAX's collectives and lax.ppermute only.
A program may use at most 64 MiB of HBM per device.

```python
import jax
import jax.numpy as jnp
from jax import lax

D = 3584
HEADS = 4
RANK = 128
GROUP = 16
LEN = 512
ROLL = 64
GROUPS = 4


def draw_group_of(key, part):
    order = jax.random.permutation(key, ROLL)
    return (order // GROUP).astype(jnp.int32)


def place_ends(result, own_key, smallest, high):
    extent = result.shape
    spot = [jax.random.randint(jax.random.fold_in(own_key, axis), (), 0, extent[axis]) for axis in range(len(extent))]
    result = result.at[tuple(spot)].set(smallest)
    longest = extent.index(max(extent))
    spot[longest] = (spot[longest] + 1) % extent[longest]
    return result.at[tuple(spot)].set(high)


def block_scale(rng, extent, split, least, top_value):
    def one(dim, blocks):
        draws = jax.random.uniform(jax.random.fold_in(jax.random.fold_in(rng, 6), dim), (blocks,), jnp.float32, least / len(split), top_value / len(split))
        return jnp.repeat(jnp.exp(draws), extent[dim] // blocks).reshape((-1,) + (1,) * (len(extent) - dim - 1))

    loudness = one(*split[0])
    for cut in split[1:]:
        loudness = loudness * one(*cut)
    return loudness


def gaussian(stream_key, extent, width, reach, pieces=(), held_as=jnp.bfloat16):
    result = jax.random.normal(stream_key, extent, jnp.float32) * width
    if len(pieces) > 0:
        result = block_scale(stream_key, extent, pieces, -0.22, 0.18) * result
    return jnp.clip(result, min=-reach, max=reach).astype(held_as)


def setup_inputs(seed: int = 0) -> dict:
    key_list = jax.random.split(jax.random.key(seed), 8)
    hidden = gaussian(key_list[0], (ROLL, LEN, D), 1.0, 6.0, ((0, 32),))
    head_proj = gaussian(key_list[1], (HEADS, D, RANK), D ** -0.5, 0.09375, ((0, 2),))
    head_out = gaussian(key_list[2], (HEADS, RANK), 0.15, 0.8984375, ((0, 2),))
    head_ratio = place_ends(jax.random.randint(key_list[3], (HEADS,), 2, 8), jax.random.fold_in(key_list[3], 1), 2, 7).astype(jnp.int32)
    group_of = draw_group_of(jax.random.fold_in(key_list[7], 71), 0)
    lengths = place_ends(jax.random.randint(key_list[5], (ROLL,), 1, LEN + 1), jax.random.fold_in(key_list[5], 1), 1, LEN).astype(jnp.int32)
    token_mask = place_ends((jax.random.randint(key_list[6], (ROLL, LEN), 0, 4) < 3).astype(jnp.int32), jax.random.fold_in(key_list[6], 1), 0, 1)
    return dict(hidden=hidden, head_proj=head_proj, head_out=head_out, head_ratio=head_ratio, group_of=group_of, lengths=lengths, token_mask=token_mask)


token_weight = 0.5
gap_weight = 0.5
clip_limit = 2.0
var_offset = 0.04

def head_mixture(head_ratio):
    ratios = head_ratio.astype(jnp.float32)
    return ratios / jnp.sum(ratios)

def reference(hidden, head_proj, head_out, head_ratio, group_of, lengths, token_mask):
    mixture = head_mixture(head_ratio)
    proj_wide = head_proj.astype(jnp.float32)
    out_wide = head_out.astype(jnp.float32)

    def rollout_score(states):
        hidden_pre = jnp.einsum('ld,hdr->hlr', states.astype(jnp.float32), proj_wide)
        active = jnp.tanh(hidden_pre).astype(jnp.bfloat16)
        active = lax.optimization_barrier(active)
        scores = jnp.einsum('hlr,hr->hl', active.astype(jnp.float32), out_wide)
        return lax.optimization_barrier(jnp.sum(mixture[:, None] * scores, axis=0))
    combined = lax.map(rollout_score, hidden)
    positions = jnp.arange(LEN)
    last_mark = positions[None, :] == (lengths - 1)[:, None]
    reward = lax.optimization_barrier(jnp.sum(jnp.where(last_mark, combined, 0.0), axis=1))
    member = (group_of[:, None] == jnp.arange(GROUPS)[None, :]).astype(jnp.float32)
    group_mean = lax.optimization_barrier(jnp.sum(member * reward[:, None], axis=0)) / GROUP
    mean_rows = lax.optimization_barrier(jnp.sum(member * group_mean[None, :], axis=1))
    deviation = reward - mean_rows
    group_var = lax.optimization_barrier(jnp.sum(member * (deviation * deviation)[:, None], axis=0)) / GROUP
    group_best = lax.optimization_barrier(jnp.max(jnp.where(member > 0, reward[:, None], -jnp.inf), axis=0))
    var_rows = lax.optimization_barrier(jnp.sum(member * group_var[None, :], axis=1))
    best_rows = lax.optimization_barrier(jnp.sum(member * group_best[None, :], axis=1))
    shaped = (deviation / jnp.sqrt(var_rows + var_offset))[:, None] + token_weight * combined - gap_weight * (best_rows - reward)[:, None]
    valid_mask = (positions[None, :] < lengths[:, None]) & (token_mask == 1)
    return jnp.where(valid_mask, jnp.clip(shaped, -clip_limit, clip_limit), 0.0)
```

```python
import functools

import jax
import jax.numpy as jnp
from jax import lax
from jax.experimental import pallas as pl
from jax.experimental.pallas import tpu as pltpu
from jax.sharding import PartitionSpec as P

GROUP = 16
LANES = 128
ROWS = 16
VMEM_BYTES = 24 << 20

token_weight = 0.5
gap_weight = 0.5
clip_limit = 2.0
var_offset = 0.04

AXES = ("dp", "head")


def tile_rows(seq_len):
    for rows in (256, 128):
        if seq_len % rows == 0:
            return rows
    return seq_len


def tile_scores(states, proj_ref, out_ref, ratio_ref, owner):
    heads = proj_ref.shape[0]
    weights = jnp.concatenate([proj_ref[k] for k in range(heads)], axis=1)
    inner = jnp.dot(states, weights, preferred_element_type=jnp.float32)
    active = jnp.tanh(inner).astype(jnp.bfloat16)
    rank = out_ref.shape[1]
    row = lax.broadcasted_iota(jnp.int32, (ROWS, rank), 0)
    readout = jnp.concatenate(
        [
            jnp.where(row == k, out_ref[k : k + 1, :].astype(jnp.float32), 0.0)
            for k in range(heads)
        ],
        axis=1,
    ).astype(jnp.bfloat16)
    scores = lax.dot_general(
        readout, active, (((1,), (1,)), ((), ())), preferred_element_type=jnp.float32
    )
    total = ratio_ref[0]
    for k in range(1, ratio_ref.shape[0]):
        total = total + ratio_ref[k]
    shape = (1, states.shape[0])
    whole = jnp.full(shape, total, jnp.int32).astype(jnp.float32)
    combined = None
    for k in range(heads):
        share = jnp.full(shape, ratio_ref[owner * heads + k], jnp.int32).astype(jnp.float32)
        term = (share / whole) * scores[k : k + 1, :]
        combined = term if combined is None else combined + term
    return combined


def first_kernel(ratio_ref, hidden_ref, proj_ref, out_ref, part_ref):
    owner = lax.axis_index("head")
    part_ref[...] = tile_scores(hidden_ref[...], proj_ref, out_ref, ratio_ref, owner)


def last_kernel(
    head_size, ratio_ref, group_ref, length_ref, hidden_ref, proj_ref, out_ref, part_ref,
    comb_ref, send_ref,
):
    roll, tile = pl.program_id(0), pl.program_id(1)
    rollouts = pl.num_programs(0)
    head = lax.axis_index("head")
    owner = lax.rem(head + head_size - 1, head_size)
    combined = part_ref[...] + tile_scores(
        hidden_ref[...], proj_ref, out_ref, ratio_ref, owner
    )
    comb_ref[...] = combined
    half = (send_ref.shape[0], 1, LANES)
    lane = lax.broadcasted_iota(jnp.int32, half, 2)

    @pl.when(tile == 0)
    def _():
        me = lax.axis_index("dp") * head_size + head
        mine = jnp.full(half, group_ref[me * rollouts + roll], jnp.int32).astype(jnp.float32)

        @pl.when(roll == 0)
        def _():
            send_ref[:, :, :LANES] = jnp.zeros(half, jnp.float32)
            send_ref[:, :, LANES:] = jnp.full(half, -1.0, jnp.float32)

        send_ref[:, :, LANES:] = jnp.where(lane == roll, mine, send_ref[:, :, LANES:])

    rows = combined.shape[1]
    position = lax.broadcasted_iota(jnp.int32, combined.shape, 1) + tile * rows
    picked = jnp.sum(
        jnp.where(position == length_ref[roll] - 1, combined, 0.0), axis=1, keepdims=True
    )
    send_ref[:, :, :LANES] += jnp.where(lane == roll, picked[None], 0.0)


def finish_kernel(
    head_size, group_ref, length_ref, every_ref, comb_ref, mask_ref, adv_ref
):
    rollouts, _, seq_len = comb_ref.shape
    me = lax.axis_index("dp") * head_size + lax.axis_index("head")
    everyone = every_ref[:, :, :LANES]
    labels = every_ref[:, :, LANES:]

    def over_all(values, op):
        return op(op(values, axis=0), axis=1, keepdims=True)

    position = lax.broadcasted_iota(jnp.int32, (1, seq_len), 1)
    for j in range(rollouts):
        combined = comb_ref[j]
        length = length_ref[j]
        reward = jnp.sum(
            jnp.where(position == length - 1, combined, 0.0), axis=1, keepdims=True
        )
        group = jnp.full(labels.shape, group_ref[me * rollouts + j], jnp.int32)
        member = labels == group.astype(jnp.float32)
        mean = over_all(jnp.where(member, everyone, 0.0), jnp.sum) / GROUP
        gap = everyone - mean[None]
        var = over_all(jnp.where(member, gap * gap, 0.0), jnp.sum) / GROUP
        best = over_all(jnp.where(member, everyone, -jnp.inf), jnp.max)
        base = (reward - mean) / jnp.sqrt(var + var_offset) - gap_weight * (best - reward)
        shaped = jnp.clip(token_weight * combined + base, -clip_limit, clip_limit)
        valid = (position < length) & (mask_ref[j : j + 1, :] == 1)
        adv_ref[j : j + 1, :] = jnp.where(valid, shaped, 0.0)


def smem():
    return pl.BlockSpec(memory_space=pltpu.SMEM)


def vmem():
    return pl.BlockSpec(memory_space=pltpu.VMEM)


def body(dp_size, head_size, hidden, head_proj, head_out, head_ratio, group_of, lengths, token_mask):
    rollouts, seq_len, width = hidden.shape
    heads, _, rank = head_proj.shape
    devices = dp_size * head_size
    rows = tile_rows(seq_len)
    grid = (rollouts, seq_len // rows)

    turn = [
        (d * head_size + h, d * head_size + (h + 1) % head_size)
        for d in range(dp_size)
        for h in range(head_size)
    ]
    other_proj = lax.ppermute(head_proj, AXES, turn)
    other_out = lax.ppermute(head_out, AXES, turn)

    states = pl.BlockSpec((None, rows, width), lambda r, t: (r, t, 0))
    projection = pl.BlockSpec((heads, width, rank), lambda r, t: (0, 0, 0))
    readout = pl.BlockSpec((heads, rank), lambda r, t: (0, 0))
    line = pl.BlockSpec((None, 1, rows), lambda r, t: (r, 0, t))
    line_shape = jax.ShapeDtypeStruct((rollouts, 1, seq_len), jnp.float32)
    tokens = rollouts * seq_len
    cost = pl.CostEstimate(
        flops=2 * tokens * width * heads * rank,
        bytes_accessed=2 * (tokens * width + heads * width * rank),
        transcendentals=tokens * heads * rank,
    )
    params = pltpu.CompilerParams(dimension_semantics=("arbitrary", "arbitrary"), vmem_limit_bytes=VMEM_BYTES
    )
    part = pl.pallas_call(
        first_kernel,
        grid=grid,
        in_specs=[smem(), states, projection, readout],
        out_specs=line,
        out_shape=line_shape,
        cost_estimate=cost,
        compiler_params=params,
        name="own_heads",
    )(head_ratio, hidden, head_proj, head_out)
    combined, send = pl.pallas_call(
        functools.partial(last_kernel, head_size),
        grid=grid,
        in_specs=[smem(), smem(), smem(), states, projection, readout, line],
        out_specs=[line, pl.BlockSpec((devices, 1, 2 * LANES), lambda r, t: (0, 0, 0))],
        out_shape=[line_shape, jax.ShapeDtypeStruct((devices, 1, 2 * LANES), jnp.float32)],
        cost_estimate=cost,
        compiler_params=params,
        name="other_heads",
    )(head_ratio, group_of, lengths, hidden, other_proj, other_out, part)
    everyone = lax.all_to_all(send, AXES, split_axis=0, concat_axis=0, tiled=True)
    return pl.pallas_call(
        functools.partial(finish_kernel, head_size),
        in_specs=[smem(), smem(), vmem(), vmem(), vmem()],
        out_specs=vmem(),
        out_shape=jax.ShapeDtypeStruct((rollouts, seq_len), jnp.float32),
        compiler_params=pltpu.CompilerParams(vmem_limit_bytes=VMEM_BYTES),
        name="advantages",
    )(group_of, lengths, everyone, combined, token_mask)


def solution(mesh):
    dp_size, head_size = mesh.shape["dp"], mesh.shape["head"]
    assert head_size == 2
    return jax.shard_map(
        functools.partial(body, dp_size, head_size),
        mesh=mesh,
        in_specs=(
            P(AXES, None, None),
            P("head", None, None),
            P("head", None),
            P(),
            P(),
            P(AXES),
            P(AXES, None),
        ),
        out_specs=P(AXES, None),
        check_vma=False,
    )
```

```python
import functools

import jax
import jax.numpy as jnp
from jax import lax
from jax.experimental import pallas as pl
from jax.experimental.pallas import tpu as pltpu
from jax.sharding import PartitionSpec as P

GROUP = 16
LANES = 128
ROWS = 16
VMEM_BYTES = 28 << 20

token_weight = 0.5
gap_weight = 0.5
clip_limit = 2.0
var_offset = 0.04

AXES = ("dp", "head")


def tile_rows(seq_len):
    for rows in (512, 256, 128):
        if seq_len % rows == 0:
            return rows
    return seq_len


def tile_scores(states, proj_ref, out_ref):
    heads = proj_ref.shape[0]
    weights = jnp.concatenate([proj_ref[k] for k in range(heads)], axis=1)
    inner = jnp.dot(states, weights, preferred_element_type=jnp.float32)
    active = jnp.tanh(inner).astype(jnp.bfloat16)
    rank = out_ref.shape[1]
    row = lax.broadcasted_iota(jnp.int32, (ROWS, rank), 0)
    readout = jnp.concatenate(
        [
            jnp.where(row == k, out_ref[k : k + 1, :].astype(jnp.float32), 0.0)
            for k in range(heads)
        ],
        axis=1,
    ).astype(jnp.bfloat16)
    return lax.dot_general(
        readout, active, (((1,), (1,)), ((), ())), preferred_element_type=jnp.float32
    )


def mixed(scores, ratio_ref, owner, heads):
    total = ratio_ref[0]
    for k in range(1, ratio_ref.shape[0]):
        total = total + ratio_ref[k]
    shape = (1, scores.shape[1])
    whole = jnp.full(shape, total, jnp.int32).astype(jnp.float32)
    combined = None
    for k in range(heads):
        share = jnp.full(shape, ratio_ref[owner * heads + k], jnp.int32).astype(jnp.float32)
        term = (share / whole) * scores[k : k + 1, :]
        combined = term if combined is None else combined + term
    return combined


def first_kernel(hidden_ref, proj_ref, out_ref, part_ref):
    scores = tile_scores(hidden_ref[...], proj_ref, out_ref)
    part_ref[...] = scores[: part_ref.shape[0], :]


def last_kernel(
    head_size, ratio_ref, group_ref, length_ref, hidden_ref, proj_ref, out_ref, part_ref,
    comb_ref, send_ref,
):
    roll, tile = pl.program_id(0), pl.program_id(1)
    rollouts = pl.num_programs(0)
    head = lax.axis_index("head")
    owner = lax.rem(head + head_size - 1, head_size)
    heads = proj_ref.shape[0]
    scores = tile_scores(hidden_ref[...], proj_ref, out_ref)
    combined = mixed(part_ref[...], ratio_ref, head, heads)
    combined = combined + mixed(scores, ratio_ref, owner, heads)
    comb_ref[...] = combined
    half = (send_ref.shape[0], 1, LANES)
    lane = lax.broadcasted_iota(jnp.int32, half, 2)

    @pl.when(tile == 0)
    def _():
        me = lax.axis_index("dp") * head_size + head
        mine = jnp.full(half, group_ref[me * rollouts + roll], jnp.int32).astype(jnp.float32)

        @pl.when(roll == 0)
        def _():
            send_ref[:, :, :LANES] = jnp.zeros(half, jnp.float32)
            send_ref[:, :, LANES:] = jnp.full(half, -1.0, jnp.float32)

        send_ref[:, :, LANES:] = jnp.where(lane == roll, mine, send_ref[:, :, LANES:])

    rows = combined.shape[1]
    position = lax.broadcasted_iota(jnp.int32, combined.shape, 1) + tile * rows
    picked = jnp.sum(
        jnp.where(position == length_ref[roll] - 1, combined, 0.0), axis=1, keepdims=True
    )
    send_ref[:, :, :LANES] += jnp.where(lane == roll, picked[None], 0.0)


def finish_kernel(
    head_size, group_ref, length_ref, every_ref, comb_ref, mask_ref, adv_ref
):
    rollouts, _, seq_len = comb_ref.shape
    me = lax.axis_index("dp") * head_size + lax.axis_index("head")
    everyone = every_ref[:, :, :LANES]
    labels = every_ref[:, :, LANES:]

    def over_all(values, op):
        return op(op(values, axis=0), axis=1, keepdims=True)

    position = lax.broadcasted_iota(jnp.int32, (1, seq_len), 1)
    for j in range(rollouts):
        combined = comb_ref[j]
        length = length_ref[j]
        reward = jnp.sum(
            jnp.where(position == length - 1, combined, 0.0), axis=1, keepdims=True
        )
        group = jnp.full(labels.shape, group_ref[me * rollouts + j], jnp.int32)
        member = labels == group.astype(jnp.float32)
        mean = over_all(jnp.where(member, everyone, 0.0), jnp.sum) / GROUP
        gap = everyone - mean[None]
        var = over_all(jnp.where(member, gap * gap, 0.0), jnp.sum) / GROUP
        best = over_all(jnp.where(member, everyone, -jnp.inf), jnp.max)
        base = (reward - mean) / jnp.sqrt(var + var_offset) - gap_weight * (best - reward)
        shaped = jnp.clip(token_weight * combined + base, -clip_limit, clip_limit)
        valid = (position < length) & (mask_ref[j : j + 1, :] == 1)
        adv_ref[j : j + 1, :] = jnp.where(valid, shaped, 0.0)


def smem():
    return pl.BlockSpec(memory_space=pltpu.SMEM)


def vmem():
    return pl.BlockSpec(memory_space=pltpu.VMEM)


def body(dp_size, head_size, hidden, head_proj, head_out, head_ratio, group_of, lengths, token_mask):
    rollouts, seq_len, width = hidden.shape
    heads, _, rank = head_proj.shape
    devices = dp_size * head_size
    rows = tile_rows(seq_len)
    grid = (rollouts, seq_len // rows)

    turn = [
        (d * head_size + h, d * head_size + (h + 1) % head_size)
        for d in range(dp_size)
        for h in range(head_size)
    ]
    other_proj = lax.ppermute(head_proj, AXES, turn)
    other_out = lax.ppermute(head_out, AXES, turn)

    states = pl.BlockSpec((None, rows, width), lambda r, t: (r, t, 0))
    projection = pl.BlockSpec((heads, width, rank), lambda r, t: (0, 0, 0))
    readout = pl.BlockSpec((heads, rank), lambda r, t: (0, 0))
    line = pl.BlockSpec((None, 1, rows), lambda r, t: (r, 0, t))
    part_line = pl.BlockSpec((None, heads, rows), lambda r, t: (r, 0, t))
    line_shape = jax.ShapeDtypeStruct((rollouts, 1, seq_len), jnp.float32)
    tokens = rollouts * seq_len
    cost = pl.CostEstimate(
        flops=2 * tokens * width * heads * rank,
        bytes_accessed=2 * (tokens * width + heads * width * rank),
        transcendentals=tokens * heads * rank,
    )
    params = pltpu.CompilerParams(dimension_semantics=("arbitrary", "arbitrary"), vmem_limit_bytes=VMEM_BYTES
    )
    part = pl.pallas_call(
        first_kernel,
        grid=grid,
        in_specs=[states, projection, readout],
        out_specs=part_line,
        out_shape=jax.ShapeDtypeStruct((rollouts, heads, seq_len), jnp.float32),
        cost_estimate=cost,
        compiler_params=params,
        name="own_heads",
    )(hidden, head_proj, head_out)
    combined, send = pl.pallas_call(
        functools.partial(last_kernel, head_size),
        grid=grid,
        in_specs=[smem(), smem(), smem(), states, projection, readout, part_line],
        out_specs=[line, pl.BlockSpec((devices, 1, 2 * LANES), lambda r, t: (0, 0, 0))],
        out_shape=[line_shape, jax.ShapeDtypeStruct((devices, 1, 2 * LANES), jnp.float32)],
        cost_estimate=cost,
        compiler_params=params,
        name="other_heads",
    )(head_ratio, group_of, lengths, hidden, other_proj, other_out, part)
    everyone = lax.all_to_all(send, AXES, split_axis=0, concat_axis=0, tiled=True)
    return pl.pallas_call(
        functools.partial(finish_kernel, head_size),
        in_specs=[smem(), smem(), vmem(), vmem(), vmem()],
        out_specs=vmem(),
        out_shape=jax.ShapeDtypeStruct((rollouts, seq_len), jnp.float32),
        compiler_params=pltpu.CompilerParams(vmem_limit_bytes=VMEM_BYTES),
        name="advantages",
    )(group_of, lengths, everyone, combined, token_mask)


def solution(mesh):
    dp_size, head_size = mesh.shape["dp"], mesh.shape["head"]
    assert head_size == 2
    return jax.shard_map(
        functools.partial(body, dp_size, head_size),
        mesh=mesh,
        in_specs=(
            P(AXES, None, None),
            P("head", None, None),
            P("head", None),
            P(),
            P(),
            P(AXES),
            P(AXES, None),
        ),
        out_specs=P(AXES, None),
        check_vma=False,
    )
```

```python
import functools

import jax
import jax.numpy as jnp
from jax import lax
from jax.experimental import pallas as pl
from jax.experimental.pallas import tpu as pltpu
from jax.sharding import PartitionSpec as P

GROUP = 16
LANES = 128
ROWS = 16
VMEM_BYTES = 28 << 20
OWN_BYTES = 55600 << 10

token_weight = 0.5
gap_weight = 0.5
clip_limit = 2.0
var_offset = 0.04

AXES = ("dp", "head")


def tile_rows(seq_len):
    for rows in (512, 256, 128):
        if seq_len % rows == 0:
            return rows
    return seq_len


def tile_scores(states, proj_ref, out_ref):
    heads = proj_ref.shape[0]
    weights = jnp.concatenate([proj_ref[k] for k in range(heads)], axis=1)
    inner = jnp.dot(states, weights, preferred_element_type=jnp.float32)
    active = jnp.tanh(inner).astype(jnp.bfloat16)
    rank = out_ref.shape[1]
    row = lax.broadcasted_iota(jnp.int32, (ROWS, rank), 0)
    readout = jnp.concatenate(
        [
            jnp.where(row == k, out_ref[k : k + 1, :].astype(jnp.float32), 0.0)
            for k in range(heads)
        ],
        axis=1,
    ).astype(jnp.bfloat16)
    return lax.dot_general(
        readout, active, (((1,), (1,)), ((), ())), preferred_element_type=jnp.float32
    )


def mixed(scores, ratio_ref, owner, heads):
    total = ratio_ref[0]
    for k in range(1, ratio_ref.shape[0]):
        total = total + ratio_ref[k]
    shape = (1, scores.shape[1])
    whole = jnp.full(shape, total, jnp.int32).astype(jnp.float32)
    combined = None
    for k in range(heads):
        share = jnp.full(shape, ratio_ref[owner * heads + k], jnp.int32).astype(jnp.float32)
        term = (share / whole) * scores[k : k + 1, :]
        combined = term if combined is None else combined + term
    return combined


def first_kernel(hidden_ref, proj_ref, out_ref, part_ref):
    scores = tile_scores(hidden_ref[...], proj_ref, out_ref)
    part_ref[...] = scores[: part_ref.shape[0], :]


def last_kernel(
    head_size, ratio_ref, group_ref, length_ref, hidden_ref, proj_ref, out_ref, part_ref,
    comb_ref, send_ref,
):
    roll, tile = pl.program_id(0), pl.program_id(1)
    rollouts = pl.num_programs(0)
    head = lax.axis_index("head")
    owner = lax.rem(head + head_size - 1, head_size)
    heads = proj_ref.shape[0]
    scores = tile_scores(hidden_ref[...], proj_ref, out_ref)
    combined = mixed(part_ref[...], ratio_ref, head, heads)
    combined = combined + mixed(scores, ratio_ref, owner, heads)
    comb_ref[...] = combined
    half = (send_ref.shape[0], 1, LANES)
    lane = lax.broadcasted_iota(jnp.int32, half, 2)

    @pl.when(tile == 0)
    def _():
        me = lax.axis_index("dp") * head_size + head
        mine = jnp.full(half, group_ref[me * rollouts + roll], jnp.int32).astype(jnp.float32)

        @pl.when(roll == 0)
        def _():
            send_ref[:, :, :LANES] = jnp.zeros(half, jnp.float32)
            send_ref[:, :, LANES:] = jnp.full(half, -1.0, jnp.float32)

        send_ref[:, :, LANES:] = jnp.where(lane == roll, mine, send_ref[:, :, LANES:])

    rows = combined.shape[1]
    position = lax.broadcasted_iota(jnp.int32, combined.shape, 1) + tile * rows
    picked = jnp.sum(
        jnp.where(position == length_ref[roll] - 1, combined, 0.0), axis=1, keepdims=True
    )
    send_ref[:, :, :LANES] += jnp.where(lane == roll, picked[None], 0.0)


def finish_kernel(
    head_size, group_ref, length_ref, every_ref, comb_ref, mask_ref, adv_ref
):
    rollouts, _, seq_len = comb_ref.shape
    me = lax.axis_index("dp") * head_size + lax.axis_index("head")
    everyone = every_ref[:, :, :LANES]
    labels = every_ref[:, :, LANES:]

    def over_all(values, op):
        return op(op(values, axis=0), axis=1, keepdims=True)

    position = lax.broadcasted_iota(jnp.int32, (1, seq_len), 1)
    for j in range(rollouts):
        combined = comb_ref[j]
        length = length_ref[j]
        reward = jnp.sum(
            jnp.where(position == length - 1, combined, 0.0), axis=1, keepdims=True
        )
        group = jnp.full(labels.shape, group_ref[me * rollouts + j], jnp.int32)
        member = labels == group.astype(jnp.float32)
        mean = over_all(jnp.where(member, everyone, 0.0), jnp.sum) / GROUP
        gap = everyone - mean[None]
        var = over_all(jnp.where(member, gap * gap, 0.0), jnp.sum) / GROUP
        best = over_all(jnp.where(member, everyone, -jnp.inf), jnp.max)
        base = (reward - mean) / jnp.sqrt(var + var_offset) - gap_weight * (best - reward)
        shaped = jnp.clip(token_weight * combined + base, -clip_limit, clip_limit)
        valid = (position < length) & (mask_ref[j : j + 1, :] == 1)
        adv_ref[j : j + 1, :] = jnp.where(valid, shaped, 0.0)


def smem():
    return pl.BlockSpec(memory_space=pltpu.SMEM)


def vmem():
    return pl.BlockSpec(memory_space=pltpu.VMEM)


def body(dp_size, head_size, hidden, head_proj, head_out, head_ratio, group_of, lengths, token_mask):
    rollouts, seq_len, width = hidden.shape
    heads, _, rank = head_proj.shape
    devices = dp_size * head_size
    rows = tile_rows(seq_len)
    grid = (rollouts, seq_len // rows)

    turn = [
        (d * head_size + h, d * head_size + (h + 1) % head_size)
        for d in range(dp_size)
        for h in range(head_size)
    ]
    other_proj = lax.ppermute(head_proj, AXES, turn)
    other_out = lax.ppermute(head_out, AXES, turn)

    states = pl.BlockSpec((None, rows, width), lambda r, t: (r, t, 0))
    projection = pl.BlockSpec((heads, width, rank), lambda r, t: (0, 0, 0))
    readout = pl.BlockSpec((heads, rank), lambda r, t: (0, 0))
    line = pl.BlockSpec((None, 1, rows), lambda r, t: (r, 0, t))
    part_line = pl.BlockSpec((None, heads, rows), lambda r, t: (r, 0, t))
    line_shape = jax.ShapeDtypeStruct((rollouts, 1, seq_len), jnp.float32)
    tokens = rollouts * seq_len
    cost = pl.CostEstimate(
        flops=2 * tokens * width * heads * rank,
        bytes_accessed=2 * (tokens * width + heads * width * rank),
        transcendentals=tokens * heads * rank,
    )
    params = pltpu.CompilerParams(dimension_semantics=("arbitrary", "arbitrary"), vmem_limit_bytes=VMEM_BYTES
    )
    part = pl.pallas_call(
        first_kernel,
        grid=grid,
        in_specs=[states, projection, readout],
        out_specs=part_line,
        out_shape=jax.ShapeDtypeStruct((rollouts, heads, seq_len), jnp.float32),
        cost_estimate=cost,
        compiler_params=pltpu.CompilerParams(
            dimension_semantics=("arbitrary", "arbitrary"), vmem_limit_bytes=OWN_BYTES
        ),
        name="own_heads",
    )(hidden, head_proj, head_out)
    combined, send = pl.pallas_call(
        functools.partial(last_kernel, head_size),
        grid=grid,
        in_specs=[smem(), smem(), smem(), states, projection, readout, part_line],
        out_specs=[line, pl.BlockSpec((devices, 1, 2 * LANES), lambda r, t: (0, 0, 0))],
        out_shape=[line_shape, jax.ShapeDtypeStruct((devices, 1, 2 * LANES), jnp.float32)],
        cost_estimate=cost,
        compiler_params=params,
        name="other_heads",
    )(head_ratio, group_of, lengths, hidden, other_proj, other_out, part)
    everyone = lax.all_to_all(send, AXES, split_axis=0, concat_axis=0, tiled=True)
    return pl.pallas_call(
        functools.partial(finish_kernel, head_size),
        in_specs=[smem(), smem(), vmem(), vmem(), vmem()],
        out_specs=vmem(),
        out_shape=jax.ShapeDtypeStruct((rollouts, seq_len), jnp.float32),
        compiler_params=pltpu.CompilerParams(vmem_limit_bytes=VMEM_BYTES),
        name="advantages",
    )(group_of, lengths, everyone, combined, token_mask)


def solution(mesh):
    dp_size, head_size = mesh.shape["dp"], mesh.shape["head"]
    assert head_size == 2
    return jax.shard_map(
        functools.partial(body, dp_size, head_size),
        mesh=mesh,
        in_specs=(
            P(AXES, None, None),
            P("head", None, None),
            P("head", None),
            P(),
            P(),
            P(AXES),
            P(AXES, None),
        ),
        out_specs=P(AXES, None),
        check_vma=False,
    )
```
